8 devices in a mesh: data: 4 (over z, y, x), stage: 2 (over core).
Axes of the slice: x: 2, y: 2, z: 1, core: 2. Of those that a mesh axis runs over, the one named last changes fastest.
Arguments:
- w_up: float32 [2, 2, 1024, 4096], P(None, 'stage')
- w_down: float32 [2, 2, 4096, 1024], P(None, 'stage')
- m_up: float32 [2, 2, 1024, 4096], P(None, 'stage')
- m_down: float32 [2, 2, 4096, 1024], P(None, 'stage')
- v_up: float32 [2, 2, 1024, 4096], P(None, 'stage')
- v_down: float32 [2, 2, 4096, 1024], P(None, 'stage')
- g_up: float32 [4, 2, 2, 1024, 4096], P('data', None, 'stage')
- g_down: float32 [4, 2, 2, 4096, 1024], P('data', None, 'stage')
- act_stash: bfloat16 [2, 2, 3072, 1024], P(None, 'stage', 'data')
- dy_last: bfloat16 [3072, 1024], P('data')
- x_next: bfloat16 [16, 3072, 1024], P(None, 'data')
- max_norm: float32 [1], replicated
Outputs:
- output 1: float32 [2, 2, 1024, 4096], P(None, 'stage')
- output 2: float32 [2, 2, 4096, 1024], P(None, 'stage')
- output 3: float32 [2, 2, 1024, 4096], P(None, 'stage')
- output 4: float32 [2, 2, 4096, 1024], P(None, 'stage')
- output 5: float32 [2, 2, 1024, 4096], P(None, 'stage')
- output 6: float32 [2, 2, 4096, 1024], P(None, 'stage')
- output 7: bfloat16 [16, 3072, 1024], P(None, 'data')
All inputs are finite; a program needn't handle non-finite values.
Results may differ from the reference program's by a relative error of at most 0.00913332.
Values are sent between devices in bfloat16 or wider.
A program may use at most 2 GiB of HBM per device.

```python
import jax
import jax.numpy as jnp
from jax import lax

D = 1024
FF = 4096
STAGES = 2
REPLICAS = 4
TOK = 768
MICRO = 16

CHUNKS = 2 * STAGES
ROWS = REPLICAS * TOK
LR = 0.002
BETA1 = 0.9
BETA2 = 0.95
ADAM_EPS = 1e-8
WDECAY = 0.1
BIAS_ONE = 1.0 - BETA1 ** 10
BIAS_TWO = 1.0 - BETA2 ** 10


def gelu_tanh(pre_act):
    return jax.nn.gelu(pre_act, approximate=True)


def layer_forward(act_in, w_in, w_out):
    pre_act = jnp.dot(act_in, w_in, preferred_element_type=jnp.float32)
    hidden = gelu_tanh(pre_act).astype(jnp.bfloat16)
    branch = jnp.dot(hidden, w_out, preferred_element_type=jnp.float32)
    return (act_in.astype(jnp.float32) + branch).astype(jnp.bfloat16)


def layer_backward(act_in, grad_y, w_in, w_out):
    pre_act = jnp.dot(act_in, w_in, preferred_element_type=jnp.float32)
    hidden, gelu_pull = jax.vjp(gelu_tanh, pre_act)
    hidden_b = hidden.astype(jnp.bfloat16)
    d_out = jnp.dot(hidden_b.T, grad_y, preferred_element_type=jnp.float32)
    d_hid = jnp.dot(grad_y, w_out.T, preferred_element_type=jnp.float32)
    d_pre = gelu_pull(d_hid)[0].astype(jnp.bfloat16)
    d_in = jnp.dot(act_in.T, d_pre, preferred_element_type=jnp.float32)
    back_rows = jnp.dot(d_pre, w_in.T, preferred_element_type=jnp.float32)
    grad_x = (grad_y.astype(jnp.float32) + back_rows).astype(jnp.bfloat16)
    return grad_x, d_in, d_out


def backward_all(stash_rows, dy_rows, old_up, old_down):
    def step_back(grad_y, layer_in):
        grad_x, d_in, d_out = layer_backward(layer_in[0], grad_y, layer_in[1], layer_in[2])
        return grad_x, (d_in, d_out)
    grad_bottom, grads = lax.scan(step_back, dy_rows, (stash_rows, old_up, old_down), reverse=True)
    return grads


def forward_all(x_next, new_up_b, new_down_b):
    batches = x_next.reshape(MICRO * REPLICAS, TOK, D)
    def run_rows(act_rows):
        def step_fwd(act_in, weights):
            return layer_forward(act_in, weights[0], weights[1]), None
        return lax.scan(step_fwd, act_rows, (new_up_b, new_down_b))[0]
    return lax.map(run_rows, batches).reshape(MICRO, ROWS, D)


def adamw_update(weight, mom, vel, grad):
    mom_new = BETA1 * mom + (1.0 - BETA1) * grad
    vel_new = BETA2 * vel + (1.0 - BETA2) * grad * grad
    step_dir = (mom_new / BIAS_ONE) / (jnp.sqrt(vel_new / BIAS_TWO) + ADAM_EPS)
    return weight - LR * (step_dir + WDECAY * weight), mom_new, vel_new


def setup_inputs(seed: int = 0) -> dict:
    root_key = jax.random.key(seed)
    sub_keys = jax.random.split(root_key, 12)
    w_up = jax.random.normal(sub_keys[0], (2, STAGES, D, FF), jnp.float32) * D ** -0.5
    w_down = jax.random.normal(sub_keys[1], (2, STAGES, FF, D), jnp.float32) * (FF * CHUNKS) ** -0.5
    act_stash = jax.random.normal(sub_keys[2], (2, STAGES, ROWS, D), jnp.float32).astype(jnp.bfloat16)
    dy_last = jax.random.normal(sub_keys[3], (ROWS, D), jnp.float32).astype(jnp.bfloat16)
    x_next = jax.random.normal(sub_keys[4], (MICRO, ROWS, D), jnp.float32).astype(jnp.bfloat16)
    d_in, d_out = backward_all(act_stash.reshape(CHUNKS, ROWS, D), dy_last, w_up.reshape(CHUNKS, D, FF).astype(jnp.bfloat16), w_down.reshape(CHUNKS, FF, D).astype(jnp.bfloat16))
    d_in = d_in.reshape(2, STAGES, D, FF)
    d_out = d_out.reshape(2, STAGES, FF, D)
    rms_in = jnp.sqrt(jnp.mean(d_in * d_in))
    rms_out = jnp.sqrt(jnp.mean(d_out * d_out))
    g_up = rms_in * (jax.random.normal(sub_keys[5], (1, 2, STAGES, D, FF), jnp.float32) / REPLICAS + jax.random.normal(sub_keys[6], (REPLICAS, 2, STAGES, D, FF), jnp.float32) * REPLICAS ** -0.5)
    g_down = rms_out * (jax.random.normal(sub_keys[7], (1, 2, STAGES, FF, D), jnp.float32) / REPLICAS + jax.random.normal(sub_keys[8], (REPLICAS, 2, STAGES, FF, D), jnp.float32) * REPLICAS ** -0.5)
    avg_in = (g_up.sum(0) + d_in) / REPLICAS
    avg_out = (g_down.sum(0) + d_out) / REPLICAS
    grad_norm = jnp.sqrt(jnp.sum(avg_in * avg_in) + jnp.sum(avg_out * avg_out))
    clip_frac = jax.random.uniform(sub_keys[9], (), jnp.float32, 0.3, 0.7)
    max_norm = (clip_frac * (grad_norm + 1e-6)).reshape(1)
    scale_in = clip_frac * jnp.sqrt(jnp.mean(avg_in * avg_in))
    scale_out = clip_frac * jnp.sqrt(jnp.mean(avg_out * avg_out))
    more_keys = jax.random.split(sub_keys[10], 4)
    m_up = 0.1 * scale_in * jax.random.normal(more_keys[0], (2, STAGES, D, FF), jnp.float32)
    m_down = 0.1 * scale_out * jax.random.normal(more_keys[1], (2, STAGES, FF, D), jnp.float32)
    v_up = 0.05 * scale_in ** 2 * (0.5 + jax.random.uniform(more_keys[2], (2, STAGES, D, FF), jnp.float32))
    v_down = 0.05 * scale_out ** 2 * (0.5 + jax.random.uniform(more_keys[3], (2, STAGES, FF, D), jnp.float32))
    return dict(w_up=w_up, w_down=w_down, m_up=m_up, m_down=m_down, v_up=v_up, v_down=v_down, g_up=g_up, g_down=g_down, act_stash=act_stash, dy_last=dy_last, x_next=x_next, max_norm=max_norm)


def reference(w_up, w_down, m_up, m_down, v_up, v_down, g_up, g_down, act_stash, dy_last, x_next, max_norm):
    old_up = w_up.reshape(CHUNKS, D, FF).astype(jnp.bfloat16)
    old_down = w_down.reshape(CHUNKS, FF, D).astype(jnp.bfloat16)
    d_in, d_out = backward_all(act_stash.reshape(CHUNKS, ROWS, D), dy_last, old_up, old_down)
    avg_in = (g_up.sum(0) + d_in.reshape(2, STAGES, D, FF)) / REPLICAS
    avg_out = (g_down.sum(0) + d_out.reshape(2, STAGES, FF, D)) / REPLICAS
    grad_norm = jnp.sqrt(jnp.sum(avg_in * avg_in) + jnp.sum(avg_out * avg_out))
    clip_coef = jnp.minimum(1.0, max_norm[0] / (grad_norm + 1e-6))
    new_up, mom_up, vel_up = adamw_update(w_up, m_up, v_up, clip_coef * avg_in)
    new_down, mom_down, vel_down = adamw_update(w_down, m_down, v_down, clip_coef * avg_out)
    y_next = forward_all(x_next, new_up.reshape(CHUNKS, D, FF).astype(jnp.bfloat16), new_down.reshape(CHUNKS, FF, D).astype(jnp.bfloat16))
    return (new_up, new_down, mom_up, mom_down, vel_up, vel_down, y_next)
```

```python
import functools

import jax
import jax.numpy as jnp
from jax import lax
from jax.experimental import pallas as pl
from jax.experimental.pallas import tpu as pltpu
from jax.sharding import PartitionSpec as P

LR = 0.002
BETA1 = 0.9
BETA2 = 0.95
ADAM_EPS = 1e-8
WDECAY = 0.1
BIAS_ONE = 1.0 - BETA1 ** 10
BIAS_TWO = 1.0 - BETA2 ** 10
CONTRACT_ROWS = (((0,), (0,)), ((), ()))
CONTRACT_LAST = (((1,), (1,)), ((), ()))
F32 = jnp.float32
BF16 = jnp.bfloat16


def gelu_tanh(pre_act):
    return jax.nn.gelu(pre_act, approximate=True)


def adamw_update(weight, mom, vel, grad):
    mom_new = BETA1 * mom + (1.0 - BETA1) * grad
    vel_new = BETA2 * vel + (1.0 - BETA2) * grad * grad
    step_dir = (mom_new / BIAS_ONE) / (jnp.sqrt(vel_new / BIAS_TWO) + ADAM_EPS)
    return weight - LR * (step_dir + WDECAY * weight), mom_new, vel_new


def adamw_body(clip, w, m, v, g, *rest):
    w_out, m_out, v_out, b_out = rest[-4:]
    new_w, new_m, new_v = adamw_update(w[0, 0], m[0, 0], v[0, 0], clip[0] * g[...])
    w_out[0, 0] = new_w
    m_out[0, 0] = new_m
    v_out[0, 0] = new_v
    b_out[...] = new_w.astype(BF16)


def adamw_call(virtual, clip, w, m, v, grad, prev):
    rows, cols = grad.shape
    block = 262144 // cols
    big = pl.BlockSpec((1, 1, block, cols), lambda i: (virtual, 0, i, 0))
    flat = pl.BlockSpec((block, cols), lambda i: (i, 0))
    in_specs = [pl.BlockSpec(memory_space=pltpu.SMEM), big, big, big, flat]
    args = [clip, w, m, v, grad]
    aliases = {}
    if prev is not None:
        in_specs += [pl.BlockSpec(memory_space=pl.ANY)] * 3
        args += list(prev)
        aliases = {5: 0, 6: 1, 7: 2}
    like = jax.ShapeDtypeStruct(w.shape, F32)
    return pl.pallas_call(
        adamw_body,
        grid=(rows // block,),
        in_specs=in_specs,
        out_specs=[big, big, big, flat],
        out_shape=[like, like, like, jax.ShapeDtypeStruct((rows, cols), BF16)],
        input_output_aliases=aliases,
        cost_estimate=pl.CostEstimate(flops=20 * rows * cols, bytes_accessed=30 * rows * cols, transcendentals=0),
        compiler_params=pltpu.CompilerParams(vmem_limit_bytes=40 * 1024 * 1024),
        name="adamw",
    )(*args)


def solution(mesh):
    replicas = mesh.shape['data']
    down_hop, up_hop, swap = [(1, 0)], [(0, 1)], [(0, 1), (1, 0)]
    w_spec = P(None, 'stage', None, None)
    g_spec = P('data', None, 'stage', None, None)
    s_spec = P(None, 'stage', 'data', None)
    dy_spec = P('data', None)
    x_spec = P(None, 'data', None)
    n_spec = P(None)

    def sharded(w_up, w_down, m_up, m_down, v_up, v_down, g_up, g_down, act_stash, dy_last, x_next, max_norm):
        pos = lax.axis_index('stage')
        rep = lax.axis_index('data')
        old_up = [w_up[v, 0].astype(BF16) for v in range(2)]
        old_down = [w_down[v, 0].astype(BF16) for v in range(2)]
        stash = [act_stash[v, 0] for v in range(2)]

        def pre_hidden(v):
            pre_act = jnp.dot(stash[v], old_up[v], preferred_element_type=F32)
            return pre_act, gelu_tanh(pre_act).astype(BF16)

        def chain(v, pre_act, grad_y):
            d_hid = lax.dot_general(grad_y, old_down[v], CONTRACT_LAST, preferred_element_type=F32)
            d_pre = jax.vjp(gelu_tanh, pre_act)[1](d_hid)[0].astype(BF16)
            back_rows = lax.dot_general(d_pre, old_up[v], CONTRACT_LAST, preferred_element_type=F32)
            return d_pre, (grad_y.astype(F32) + back_rows).astype(BF16)

        def backward(v, grad_top):
            pre_act, hidden = pre_hidden(v)
            zeros = (jnp.zeros(hidden.shape, BF16), jnp.zeros(grad_top.shape, BF16))
            first = lax.cond(pos == 1, lambda g: chain(v, pre_act, g), lambda g: zeros, grad_top)
            grad_mid = lax.ppermute(first[1], 'stage', down_hop)
            d_pre, grad_bottom = lax.cond(pos == 0, lambda g: chain(v, pre_act, g), lambda g: first, grad_mid)
            grad_y = jnp.where(pos == 1, grad_top, grad_mid)
            sum_down = lax.dot_general(hidden, grad_y, CONTRACT_ROWS, preferred_element_type=F32) + g_down[0, v, 0]
            part_down = lax.psum_scatter(sum_down, 'data', scatter_dimension=0, tiled=True)
            sum_up = lax.dot_general(stash[v], d_pre, CONTRACT_ROWS, preferred_element_type=F32) + g_up[0, v, 0]
            part_up = lax.psum_scatter(sum_up, 'data', scatter_dimension=0, tiled=True)
            return lax.ppermute(grad_bottom, 'stage', up_hop), part_up, part_down

        grad_flow, up1, down1 = backward(1, dy_last)
        grad_flow, up0, down0 = backward(0, grad_flow)
        up = [up0 / replicas, up1 / replicas]
        down = [down0 / replicas, down1 / replicas]

        part_sq = sum(jnp.sum(t * t) for t in up + down)
        total_sq = lax.psum(part_sq, ('data', 'stage'))
        clip = jnp.minimum(1.0, max_norm / (jnp.sqrt(total_sq) + 1e-6))

        def gather(t):
            return lax.all_gather(t, 'data', axis=0, tiled=True)

        def shard(t, like):
            rows = like.shape[0]
            return lax.dynamic_slice_in_dim(t[0, 0], rep * rows, rows, 0)

        def fresh_shard(w, m, v, grad):
            return adamw_update(shard(w, grad), shard(m, grad), shard(v, grad), clip[0] * grad)[0].astype(BF16)

        def both(t):
            other = lax.ppermute(t, 'stage', swap)
            return jnp.where(pos == 0, t, other), jnp.where(pos == 0, other, t)

        def forward(act, w_in, w_out):
            pre_act = jnp.dot(act, w_in, preferred_element_type=F32)
            hidden = gelu_tanh(pre_act).astype(BF16)
            branch = jnp.dot(hidden, w_out, preferred_element_type=F32)
            return (act.astype(F32) + branch).astype(BF16)

        n_micro, rows, width = x_next.shape
        half = n_micro // 2
        act = lax.dynamic_slice_in_dim(x_next, pos * half, half, 0).reshape(half * rows, width)

        full_down1 = gather(down[1])
        fresh_up0 = gather(fresh_shard(w_up, m_up, v_up, up[0]))
        fresh_down0 = gather(fresh_shard(w_down, m_down, v_down, down[0]))
        full_up1 = gather(up[1])
        pair_up, pair_down = both(fresh_up0), both(fresh_down0)
        for l in range(2):
            act = forward(act, pair_up[l], pair_down[l])

        *new_down, fresh_down1 = adamw_call(1, clip, w_down, m_down, v_down, full_down1, None)
        *new_up, fresh_up1 = adamw_call(1, clip, w_up, m_up, v_up, full_up1, None)
        pair_up, pair_down = both(fresh_up1), both(fresh_down1)
        full_down0 = gather(down[0])
        full_up0 = gather(up[0])
        for l in range(2):
            act = forward(act, pair_up[l], pair_down[l])
        *new_down, _ = adamw_call(0, clip, w_down, m_down, v_down, full_down0, new_down)
        *new_up, _ = adamw_call(0, clip, w_up, m_up, v_up, full_up0, new_up)

        own = act.reshape(half, rows, width)
        other = lax.ppermute(own, 'stage', swap)
        y_next = jnp.where(pos == 0, jnp.concatenate([own, other]), jnp.concatenate([other, own]))
        return (new_up[0], new_down[0], new_up[1], new_down[1], new_up[2], new_down[2], y_next)

    return jax.shard_map(sharded, mesh=mesh, in_specs=(w_spec, w_spec, w_spec, w_spec, w_spec, w_spec, g_spec, g_spec, s_spec, dy_spec, x_spec, n_spec), out_specs=(w_spec, w_spec, w_spec, w_spec, w_spec, w_spec, x_spec), check_vma=False)
```

```python
import functools

import jax
import jax.numpy as jnp
from jax import lax
from jax.experimental import pallas as pl
from jax.experimental.pallas import tpu as pltpu
from jax.sharding import PartitionSpec as P

LR = 0.002
BETA1 = 0.9
BETA2 = 0.95
ADAM_EPS = 1e-8
WDECAY = 0.1
BIAS_ONE = 1.0 - BETA1 ** 10
BIAS_TWO = 1.0 - BETA2 ** 10
CONTRACT_ROWS = (((0,), (0,)), ((), ()))
CONTRACT_LAST = (((1,), (1,)), ((), ()))
F32 = jnp.float32
BF16 = jnp.bfloat16


def gelu_tanh(pre_act):
    return jax.nn.gelu(pre_act, approximate=True)


def adamw_update(weight, mom, vel, grad):
    mom_new = BETA1 * mom + (1.0 - BETA1) * grad
    vel_new = BETA2 * vel + (1.0 - BETA2) * grad * grad
    step_dir = (mom_new / BIAS_ONE) / (jnp.sqrt(vel_new / BIAS_TWO) + ADAM_EPS)
    return weight - LR * (step_dir + WDECAY * weight), mom_new, vel_new


def adamw_body(clip, w, m, v, g, *rest):
    w_out, m_out, v_out, b_out = rest[-4:]
    new_w, new_m, new_v = adamw_update(w[0, 0], m[0, 0], v[0, 0], clip[0] * g[...])
    w_out[0, 0] = new_w
    m_out[0, 0] = new_m
    v_out[0, 0] = new_v
    b_out[...] = new_w.astype(BF16)


def adamw_call(virtual, clip, w, m, v, grad, prev):
    rows, cols = grad.shape
    block = 262144 // cols
    big = pl.BlockSpec((1, 1, block, cols), lambda i: (virtual, 0, i, 0))
    flat = pl.BlockSpec((block, cols), lambda i: (i, 0))
    in_specs = [pl.BlockSpec(memory_space=pltpu.SMEM), big, big, big, flat]
    args = [clip, w, m, v, grad]
    aliases = {}
    if prev is not None:
        in_specs += [pl.BlockSpec(memory_space=pl.ANY)] * 3
        args += list(prev)
        aliases = {5: 0, 6: 1, 7: 2}
    like = jax.ShapeDtypeStruct(w.shape, F32)
    return pl.pallas_call(
        adamw_body,
        grid=(rows // block,),
        in_specs=in_specs,
        out_specs=[big, big, big, flat],
        out_shape=[like, like, like, jax.ShapeDtypeStruct((rows, cols), BF16)],
        input_output_aliases=aliases,
        cost_estimate=pl.CostEstimate(flops=20 * rows * cols, bytes_accessed=30 * rows * cols, transcendentals=0),
        compiler_params=pltpu.CompilerParams(vmem_limit_bytes=40 * 1024 * 1024),
        name="adamw",
    )(*args)


def solution(mesh):
    replicas = mesh.shape['data']
    down_hop, up_hop, swap = [(1, 0)], [(0, 1)], [(0, 1), (1, 0)]
    w_spec = P(None, 'stage', None, None)
    g_spec = P('data', None, 'stage', None, None)
    s_spec = P(None, 'stage', 'data', None)
    dy_spec = P('data', None)
    x_spec = P(None, 'data', None)
    n_spec = P(None)

    def sharded(w_up, w_down, m_up, m_down, v_up, v_down, g_up, g_down, act_stash, dy_last, x_next, max_norm):
        pos = lax.axis_index('stage')
        rep = lax.axis_index('data')
        old_up = [w_up[v, 0].astype(BF16) for v in range(2)]
        old_down = [w_down[v, 0].astype(BF16) for v in range(2)]
        stash = [act_stash[v, 0] for v in range(2)]

        def pre_hidden(v):
            pre_act = jnp.dot(stash[v], old_up[v], preferred_element_type=F32)
            return pre_act, gelu_tanh(pre_act).astype(BF16)

        def chain(v, pre_act, grad_y):
            d_hid = lax.dot_general(grad_y, old_down[v], CONTRACT_LAST, preferred_element_type=F32)
            d_pre = jax.vjp(gelu_tanh, pre_act)[1](d_hid)[0].astype(BF16)
            back_rows = lax.dot_general(d_pre, old_up[v], CONTRACT_LAST, preferred_element_type=F32)
            return d_pre, (grad_y.astype(F32) + back_rows).astype(BF16)

        y_pos, x_pos = rep // 2, rep % 2

        def x_swap(t):
            return lax.ppermute(t, 'data', [(src, src ^ 1) for src in range(replicas)])

        def y_swap(t):
            return lax.ppermute(t, 'data', [(src, src ^ 2) for src in range(replicas)])

        def pick(t, idx, size):
            return lax.dynamic_slice_in_dim(t, idx * size, size, 0)

        def scatter(make, rows):
            quarter, eighth = rows // 4, rows // 8
            got_a = x_swap(make((1 - x_pos) * quarter, quarter))
            got_b = y_swap(make(2 * quarter + (1 - y_pos) * quarter, quarter))
            keep_a = make(x_pos * quarter, quarter)
            keep_b = make(2 * quarter + y_pos * quarter, quarter)
            send_a = pick(keep_a, 1 - y_pos, eighth) + pick(got_a, 1 - y_pos, eighth)
            send_b = pick(keep_b, 1 - x_pos, eighth) + pick(got_b, 1 - x_pos, eighth)
            more_a, more_b = y_swap(send_a), x_swap(send_b)
            own_a = pick(keep_a, y_pos, eighth) + pick(got_a, y_pos, eighth)
            own_b = pick(keep_b, x_pos, eighth) + pick(got_b, x_pos, eighth)
            return own_a + more_a, own_b + more_b

        def spread(pair):
            a, b = pair
            a_y, b_x = y_swap(a), x_swap(b)
            a_x, b_y = x_swap(a), y_swap(b)
            return [a, a_y, a_x, x_swap(a_y)], [b, b_x, b_y, y_swap(b_x)]

        def join(parts):
            parts_a, parts_b = parts
            eighth = parts_a[0].shape[0]
            full = jnp.zeros((8 * eighth,) + parts_a[0].shape[1:], parts_a[0].dtype)
            for i in range(4):
                dx, dy = i // 2, i % 2
                at = 2 * (x_pos ^ dx) + (y_pos ^ dy)
                full = lax.dynamic_update_slice_in_dim(full, parts_a[i], at * eighth, 0)
                at = 4 + 2 * (y_pos ^ dx) + (x_pos ^ dy)
                full = lax.dynamic_update_slice_in_dim(full, parts_b[i], at * eighth, 0)
            return full

        def backward(v, grad_top):
            pre_act, hidden = pre_hidden(v)
            zeros = (jnp.zeros(hidden.shape, BF16), jnp.zeros(grad_top.shape, BF16))
            first = lax.cond(pos == 1, lambda g: chain(v, pre_act, g), lambda g: zeros, grad_top)
            grad_mid = lax.ppermute(first[1], 'stage', down_hop)
            d_pre, grad_bottom = lax.cond(pos == 0, lambda g: chain(v, pre_act, g), lambda g: first, grad_mid)
            grad_y = jnp.where(pos == 1, grad_top, grad_mid)
            def make_down(start, size):
                cols = lax.dynamic_slice_in_dim(hidden, start, size, 1)
                return lax.dot_general(cols, grad_y, CONTRACT_ROWS, preferred_element_type=F32) + lax.dynamic_slice_in_dim(g_down[0, v, 0], start, size, 0)

            def make_up(start, size):
                cols = lax.dynamic_slice_in_dim(stash[v], start, size, 1)
                return lax.dot_general(cols, d_pre, CONTRACT_ROWS, preferred_element_type=F32) + lax.dynamic_slice_in_dim(g_up[0, v, 0], start, size, 0)

            part_down = scatter(make_down, hidden.shape[1])
            part_up = scatter(make_up, stash[v].shape[1])
            return lax.ppermute(grad_bottom, 'stage', up_hop), part_up, part_down

        grad_flow, up1, down1 = backward(1, dy_last)
        grad_flow, up0, down0 = backward(0, grad_flow)
        up = [[t / replicas for t in pair] for pair in (up0, up1)]
        down = [[t / replicas for t in pair] for pair in (down0, down1)]

        part_sq = sum(jnp.sum(t * t) for pair in up + down for t in pair)
        total_sq = lax.psum(part_sq, ('data', 'stage'))
        clip = jnp.minimum(1.0, max_norm / (jnp.sqrt(total_sq) + 1e-6))

        def gather(pair):
            return join(spread(pair))

        def fresh_shard(w, m, v, pair):
            eighth = pair[0].shape[0]
            made = []
            for at, grad in zip((2 * x_pos + y_pos, 4 + 2 * y_pos + x_pos), pair):
                rows = [pick(t[0, 0], at, eighth) for t in (w, m, v)]
                made.append(adamw_update(*rows, clip[0] * grad)[0].astype(BF16))
            return made

        def both(t):
            other = lax.ppermute(t, 'stage', swap)
            return jnp.where(pos == 0, t, other), jnp.where(pos == 0, other, t)

        def forward(act, w_in, w_out):
            pre_act = jnp.dot(act, w_in, preferred_element_type=F32)
            hidden = gelu_tanh(pre_act).astype(BF16)
            branch = jnp.dot(hidden, w_out, preferred_element_type=F32)
            return (act.astype(F32) + branch).astype(BF16)

        n_micro, rows, width = x_next.shape
        half = n_micro // 2
        act = lax.dynamic_slice_in_dim(x_next, pos * half, half, 0).reshape(half * rows, width)

        full_down1 = gather(down[1])
        fresh_up0 = gather(fresh_shard(w_up, m_up, v_up, up[0]))
        fresh_down0 = gather(fresh_shard(w_down, m_down, v_down, down[0]))
        full_up1 = gather(up[1])
        pair_up, pair_down = both(fresh_up0), both(fresh_down0)
        for l in range(2):
            act = forward(act, pair_up[l], pair_down[l])

        *new_down, fresh_down1 = adamw_call(1, clip, w_down, m_down, v_down, full_down1, None)
        *new_up, fresh_up1 = adamw_call(1, clip, w_up, m_up, v_up, full_up1, None)
        pair_up, pair_down = both(fresh_up1), both(fresh_down1)
        full_down0 = gather(down[0])
        full_up0 = gather(up[0])
        for l in range(2):
            act = forward(act, pair_up[l], pair_down[l])
        *new_down, _ = adamw_call(0, clip, w_down, m_down, v_down, full_down0, new_down)
        *new_up, _ = adamw_call(0, clip, w_up, m_up, v_up, full_up0, new_up)

        own = act.reshape(half, rows, width)
        other = lax.ppermute(own, 'stage', swap)
        y_next = jnp.where(pos == 0, jnp.concatenate([own, other]), jnp.concatenate([other, own]))
        return (new_up[0], new_down[0], new_up[1], new_down[1], new_up[2], new_down[2], y_next)

    return jax.shard_map(sharded, mesh=mesh, in_specs=(w_spec, w_spec, w_spec, w_spec, w_spec, w_spec, g_spec, g_spec, s_spec, dy_spec, x_spec, n_spec), out_specs=(w_spec, w_spec, w_spec, w_spec, w_spec, w_spec, x_spec), check_vma=False)
```

```python
import functools

import jax
import jax.numpy as jnp
from jax import lax
from jax.experimental import pallas as pl
from jax.experimental.pallas import tpu as pltpu
from jax.sharding import PartitionSpec as P

LR = 0.002
BETA1 = 0.9
BETA2 = 0.95
ADAM_EPS = 1e-8
WDECAY = 0.1
BIAS_ONE = 1.0 - BETA1 ** 10
BIAS_TWO = 1.0 - BETA2 ** 10
CONTRACT_ROWS = (((0,), (0,)), ((), ()))
CONTRACT_LAST = (((1,), (1,)), ((), ()))
F32 = jnp.float32
BF16 = jnp.bfloat16
D_MODEL, D_FF = 1024, 4096
ROW_TILE = 384
FF_TILE = 1024
CORE_TILES = 16
TILE = {'up': (64, D_FF), 'down': (256, D_MODEL)}
N_TILES = 16
OWN_TILES = 4
STRIP = 8


def gelu_tanh(pre_act):
    return jax.nn.gelu(pre_act, approximate=True)


def adamw_update(weight, mom, vel, grad):
    mom_new = BETA1 * mom + (1.0 - BETA1) * grad
    vel_new = BETA2 * vel + (1.0 - BETA2) * grad * grad
    step_dir = mom_new * (BIAS_TWO ** 0.5 / BIAS_ONE) / (jnp.sqrt(vel_new) + ADAM_EPS * BIAS_TWO ** 0.5)
    return weight - LR * (step_dir + WDECAY * weight), mom_new, vel_new


class Job:
    def __init__(self, kind, virtual, own):
        self.kind, self.virtual, self.own = kind, virtual, own
        self.count = OWN_TILES if own else N_TILES - OWN_TILES


class Plan:
    pass


def fused_kernel(plan, place, *refs):
    refs = list(refs)

    def take(count):
        return [refs.pop(0) for _ in range(count)]

    step = pl.program_id(0)
    slot = lax.rem(step, 2)
    pos, rep = place[0], place[1]
    clip, = take(1)
    if plan.rows:
        x_ref, *weights = take(5)
    state = {kind: take(3) for kind in plan.kinds}
    grads = {kind: take(1)[0] for kind in plan.kinds}
    take(plan.n_alias)
    y_refs = take(plan.n_act)
    outs = {kind: take(3) for kind in plan.kinds}
    fresh = {kind: take(1)[0] for kind in plan.kinds if plan.fresh}
    if plan.rows:
        w_in, w_out, hidden, w_sem = take(4)
    bufs = {kind: take(5 if plan.fresh else 4) for kind in plan.kinds}

    def rows_of(kind, job, t):
        size = TILE[kind][0]
        if job.own:
            src, dst = t, rep * OWN_TILES + t
        else:
            src = dst = lax.rem(rep * OWN_TILES + OWN_TILES + t, N_TILES)
        return pl.multiple_of(src * size, size), pl.multiple_of(dst * size, size), size

    def loads(kind, job, t, where):
        src, dst, size = rows_of(kind, job, t)
        ins, sem = bufs[kind][0], bufs[kind][-2]
        refs_in = [ref.at[job.virtual, 0, pl.ds(dst, size), :] for ref in state[kind]] + [grads[kind].at[pl.ds(src, size), :]]
        return [pltpu.make_async_copy(ref, ins.at[where, j], sem.at[where, j]) for j, ref in enumerate(refs_in)]

    def stores(kind, job, t, where):
        src, dst, size = rows_of(kind, job, t)
        made, sem = bufs[kind][1], bufs[kind][-1]
        copies = [pltpu.make_async_copy(made.at[where, j], ref.at[job.virtual, 0, pl.ds(dst, size), :], sem.at[where, j])
                  for j, ref in enumerate(outs[kind])]
        if plan.fresh:
            row = src if plan.fresh == 'own' else dst
            copies.append(pltpu.make_async_copy(bufs[kind][2].at[where], fresh[kind].at[pl.ds(row, size), :], sem.at[where, 3]))
        return copies

    def for_step(at, make, where, wait):
        for kind in plan.kinds:
            job = plan.jobs[kind]
            @pl.when((at >= 0) & (at < job.count))
            def _(kind=kind, job=job):
                for copy in make(kind, job, at, where):
                    copy.wait() if wait else copy.start()

    def fill(which):
        for j, dst in enumerate((w_in, w_out)):
            pltpu.make_async_copy(weights[2 * j + which], dst, w_sem.at[j]).start()

    @pl.when(step == 0)
    def _():
        for_step(step, loads, 0, False)
        if plan.rows:
            pl.when(pos == plan.owner)(lambda: fill(0))
            pl.when(pos != plan.owner)(lambda: fill(1))

    for_step(step + 1, loads, 1 - slot, False)
    for_step(step, loads, slot, True)
    for_step(step - 2, stores, slot, True)

    if plan.rows:
        @pl.when(step == 0)
        def _():
            for j, dst in enumerate((w_in, w_out)):
                pltpu.make_async_copy(weights[2 * j], dst, w_sem.at[j]).wait()

        for at in range(0, D_FF, FF_TILE):
            part = jnp.dot(x_ref[...], w_in[:, at:at + FF_TILE], preferred_element_type=F32)
            hidden[:, at:at + FF_TILE] = gelu_tanh(part).astype(BF16)
        out = jnp.dot(hidden[...], w_out[...], preferred_element_type=F32)
        out = (x_ref[...].astype(F32) + out).astype(BF16)
        for y_ref in y_refs:
            y_ref[...] = out

    scale = clip[0]
    for kind in plan.kinds:
        ins, made = bufs[kind][0], bufs[kind][1]
        for row in range(0, TILE[kind][0], STRIP):
            for col in range(0, TILE[kind][1], D_MODEL):
                at = (pl.ds(row, STRIP), pl.ds(col, D_MODEL))
                old = [ins[(slot, j) + at] for j in range(4)]
                new = adamw_update(old[0], old[1], old[2], scale * old[3])
                for j in range(3):
                    made[(slot, j) + at] = new[j]
                if plan.fresh:
                    bufs[kind][2][(slot,) + at] = new[0].astype(BF16)

    for_step(step, stores, slot, False)

    @pl.when(step == plan.steps - 1)
    def _():
        for_step(step - 1, stores, 1 - slot, True)
        for_step(step, stores, slot, True)


def fused_call(name, place, clip, jobs, state, grads, prev, fresh, act=None, weights=None, owner=0, first=False, last=False):
    plan = Plan()
    plan.kinds = tuple(kind for kind in ('up', 'down') if kind in jobs)
    plan.jobs, plan.owner, plan.rows, plan.fresh = jobs, owner, act is not None, fresh
    plan.steps = CORE_TILES if plan.rows else max(job.count for job in jobs.values())
    hbm = pl.BlockSpec(memory_space=pl.ANY)
    in_specs, args = [pl.BlockSpec(memory_space=pltpu.SMEM)], [clip]
    out_specs, out_shape, scratch = [], [], []
    tile = (ROW_TILE, D_MODEL)

    def here(i, place):
        return (i, 0)

    def among_both(i, place):
        return (place[0] * CORE_TILES + i, 0)

    if plan.rows:
        in_specs += [pl.BlockSpec(tile, among_both if first else here)] + [hbm] * 4
        args += [act, *weights]
        out_specs.append(pl.BlockSpec(tile, here))
        out_shape.append(jax.ShapeDtypeStruct((CORE_TILES * ROW_TILE, D_MODEL), BF16))
        if last:
            out_specs.append(pl.BlockSpec(tile, among_both))
            out_shape.append(jax.ShapeDtypeStruct((2 * CORE_TILES * ROW_TILE, D_MODEL), BF16))
        scratch += [pltpu.VMEM((D_MODEL, D_FF), BF16), pltpu.VMEM((D_FF, D_MODEL), BF16), pltpu.VMEM((ROW_TILE, D_FF), BF16), pltpu.SemaphoreType.DMA((2,))]
    plan.n_act = len(out_shape)
    for kind in plan.kinds:
        args += list(state[kind])
    args += [grads[kind] for kind in plan.kinds]
    aliases = {}
    for kind in plan.kinds:
        for j, arr in enumerate(prev.get(kind, (None,) * 3)[:3]):
            if arr is not None:
                aliases[1 + len(args)] = len(out_shape)
                args.append(arr)
            out_shape.append(jax.ShapeDtypeStruct(state[kind][j].shape, F32))
    if fresh:
        for kind in plan.kinds:
            arr = prev.get(kind, (None,) * 4)[3]
            if arr is not None and fresh != 'own':
                aliases[1 + len(args)] = len(out_shape)
                args.append(arr)
            rows, cols = state[kind][0].shape[2:]
            out_shape.append(jax.ShapeDtypeStruct((rows // 4 if fresh == 'own' else rows, cols), BF16))
    plan.n_alias = len(aliases)
    in_specs += [hbm] * (len(args) - len(in_specs))
    out_specs += [hbm] * (len(out_shape) - len(out_specs))
    for kind in plan.kinds:
        scratch += [pltpu.VMEM((2, 4) + TILE[kind], F32), pltpu.VMEM((2, 3) + TILE[kind], F32)]
        if fresh:
            scratch.append(pltpu.VMEM((2,) + TILE[kind], BF16))
        scratch += [pltpu.SemaphoreType.DMA((2, 4)), pltpu.SemaphoreType.DMA((2, 4))]
    adam = sum(job.count for job in jobs.values()) * TILE['up'][0] * D_FF
    rows = CORE_TILES * ROW_TILE if plan.rows else 0
    results = pl.pallas_call(
        functools.partial(fused_kernel, plan),
        grid_spec=pltpu.PrefetchScalarGridSpec(num_scalar_prefetch=1, grid=(plan.steps,), in_specs=in_specs, out_specs=out_specs, scratch_shapes=scratch),
        out_shape=out_shape,
        input_output_aliases=aliases,
        cost_estimate=pl.CostEstimate(flops=4 * rows * D_MODEL * D_FF + 2000 * adam, bytes_accessed=30 * adam + 4 * rows * D_MODEL, transcendentals=0),
        compiler_params=pltpu.CompilerParams(vmem_limit_bytes=58 * 1024 * 1024),
        name=name,
    )(place, *args)
    acts, results = results[:plan.n_act], results[plan.n_act:]
    n = len(plan.kinds)
    made = {kind: list(results[3 * i:3 * i + 3]) + ([results[3 * n + i]] if fresh else [None]) for i, kind in enumerate(plan.kinds)}
    return acts, made


def solution(mesh):
    replicas = mesh.shape['data']
    down_hop, up_hop, swap = [(1, 0)], [(0, 1)], [(0, 1), (1, 0)]
    w_spec = P(None, 'stage', None, None)
    g_spec = P('data', None, 'stage', None, None)
    s_spec = P(None, 'stage', 'data', None)
    dy_spec = P('data', None)
    x_spec = P(None, 'data', None)
    n_spec = P(None)

    def sharded(w_up, w_down, m_up, m_down, v_up, v_down, g_up, g_down, act_stash, dy_last, x_next, max_norm):
        pos = lax.axis_index('stage')
        rep = lax.axis_index('data')
        place = jnp.stack([pos, rep]).astype(jnp.int32)

        def backward(v, grad_top, late):
            f_up, f_down = w_up[v, 0], w_down[v, 0]
            if late is not None:
                f_up, f_down, _ = lax.optimization_barrier((f_up, f_down, late))
            old_up, old_down, stash = f_up.astype(BF16), f_down.astype(BF16), act_stash[v, 0]
            pre_act = jnp.dot(stash, old_up, preferred_element_type=F32)
            hidden = gelu_tanh(pre_act).astype(BF16)

            def chain(grad_y):
                d_hid = lax.dot_general(grad_y, old_down, CONTRACT_LAST, preferred_element_type=F32)
                d_pre = jax.vjp(gelu_tanh, pre_act)[1](d_hid)[0].astype(BF16)
                back_rows = lax.dot_general(d_pre, old_up, CONTRACT_LAST, preferred_element_type=F32)
                return d_pre, (grad_y.astype(F32) + back_rows).astype(BF16)

            zeros = (jnp.zeros(hidden.shape, BF16), jnp.zeros(grad_top.shape, BF16))
            first = lax.cond(pos == 1, chain, lambda g: zeros, grad_top)
            grad_mid = lax.ppermute(first[1], 'stage', down_hop)
            grad_y = jnp.where(pos == 1, grad_top, grad_mid)
            sum_down = lax.dot_general(hidden, grad_y, CONTRACT_ROWS, preferred_element_type=F32) + g_down[0, v, 0]
            part_down = lax.psum_scatter(sum_down, 'data', scatter_dimension=0, tiled=True)
            grad_mid, sum_down = lax.optimization_barrier((grad_mid, sum_down))
            d_pre, grad_bottom = lax.cond(pos == 0, chain, lambda g: first, grad_mid)
            sum_up = lax.dot_general(stash, d_pre, CONTRACT_ROWS, preferred_element_type=F32) + g_up[0, v, 0]
            part_up = lax.psum_scatter(sum_up, 'data', scatter_dimension=0, tiled=True)
            return lax.ppermute(grad_bottom, 'stage', up_hop), part_up, part_down, sum_down[:8, :128]

        grad_flow, up1, down1, late = backward(1, dy_last, None)
        grad_flow, up0, down0, _ = backward(0, grad_flow, late)
        up = [up0 / replicas, up1 / replicas]
        down = [down0 / replicas, down1 / replicas]

        part_sq = sum(jnp.sum(t * t) for t in up + down)
        total_sq = lax.psum(part_sq, ('data', 'stage'))
        clip = jnp.minimum(1.0, max_norm / (jnp.sqrt(total_sq) + 1e-6))

        def gather(t):
            return lax.all_gather(t, 'data', axis=0, tiled=True)

        state = {'up': (w_up, m_up, v_up), 'down': (w_down, m_down, v_down)}
        call = functools.partial(fused_call, place=place, clip=clip, state=state)
        n_micro, rows, width = x_next.shape
        half = n_micro // 2

        _, made = call('adam_own0', jobs={k: Job(k, 0, True) for k in state}, grads={'up': up[0], 'down': down[0]}, prev={}, fresh='own')
        fresh_up, fresh_down = gather(made['up'][3]), gather(made['down'][3])
        full_down1, full_up1, full_down0, full_up0 = gather(down[1]), gather(up[1]), gather(down[0]), gather(up[0])
        pair = (fresh_up, lax.ppermute(fresh_up, 'stage', swap), fresh_down, lax.ppermute(fresh_down, 'stage', swap))

        made = {k: made[k][:3] + [None] for k in made}
        (act,), made = call('fwd0', jobs={k: Job(k, 1, True) for k in state}, grads={'up': up[1], 'down': down[1]}, prev=made, fresh='all',
                            act=x_next.reshape(n_micro * rows, width), weights=pair, owner=0, first=True)
        (act,), more = call('fwd1', jobs={'down': Job('down', 1, False)}, grads={'down': full_down1}, prev=made, fresh='all', act=act, weights=pair, owner=1)
        made.update(more)
        _, more = call('adam_up1', jobs={'up': Job('up', 1, False)}, grads={'up': full_up1}, prev=made, fresh='all')
        made.update(more)
        fresh_up, fresh_down = made['up'][3], made['down'][3]
        pair = (fresh_up, lax.ppermute(fresh_up, 'stage', swap), fresh_down, lax.ppermute(fresh_down, 'stage', swap))
        (act,), _ = call('fwd2', jobs={}, grads={}, prev={}, fresh=None, act=act, weights=pair, owner=0)
        (own, y_next), more = call('fwd3', jobs={'down': Job('down', 0, False)}, grads={'down': full_down0}, prev=made, fresh=None, act=act, weights=pair, owner=1, last=True)
        made.update(more)
        other = lax.ppermute(own, 'stage', swap)
        _, more = call('adam_up0', jobs={'up': Job('up', 0, False)}, grads={'up': full_up0}, prev=made, fresh=None)
        made.update(more)
        y_next = lax.dynamic_update_slice_in_dim(y_next, other, (1 - pos) * half * rows, 0).reshape(n_micro, rows, width)
        up_new, down_new = made['up'], made['down']
        return (up_new[0], down_new[0], up_new[1], down_new[1], up_new[2], down_new[2], y_next)

    return jax.shard_map(sharded, mesh=mesh, in_specs=(w_spec, w_spec, w_spec, w_spec, w_spec, w_spec, g_spec, g_spec, s_spec, dy_spec, x_spec, n_spec), out_specs=(w_spec, w_spec, w_spec, w_spec, w_spec, w_spec, x_spec), check_vma=False)
```
